16 devices in a mesh: data: 2 (over y, z), seq: 8 (over x, core).
Axes of the slice: x: 4, y: 2, z: 1, core: 2. Of those that a mesh axis runs over, the one named last changes fastest.
The devices are a block of a 4x4x8 slice.
Arguments:
- x: bfloat16 [64, 4096, 512], P('data', 'seq'), parts along dimension 0
- w_tok1: bfloat16 [2, 4096, 256], replicated
- b_tok1: float32 [2, 256], replicated
- w_tok2: bfloat16 [2, 256, 4096], replicated
- b_tok2: float32 [2, 4096], replicated
- w_ch1: bfloat16 [2, 512, 2048], replicated
- b_ch1: float32 [2, 2048], replicated
- w_ch2: bfloat16 [2, 2048, 512], replicated
- b_ch2: float32 [2, 512], replicated
- ln_params: float32 [2, 4, 512], replicated
Outputs:
- output: bfloat16 [64, 4096, 512], P('data', 'seq'), parts along dimension 0
There are 2 independent parts. The reference program is written for one: setup_inputs(seed, part) draws one part's arguments, and reference() takes and returns one part's arrays. A program takes and returns all parts, laid end to end along the dimension named above; an argument that names none is the same for every part.
All inputs are finite; a program needn't handle non-finite values.
Results may differ from the reference program's by a relative error of at most 0.0171184.
Values are sent between devices in bfloat16 or wider.
A program may use at most 768 MiB of HBM per device.

```python
import jax
import jax.numpy as jnp
from jax import lax

BATCH = 32
PATCHES = 4096
CHANNELS = 512
TOKEN_HIDDEN = 256
CHANNEL_HIDDEN = 2048
LAYERS = 2
LN_EPS = 1e-6


def normal_weight(rng_key, arr_shape, fan_in, weight_gain):
    normals = jax.random.normal(rng_key, arr_shape, jnp.float32)
    return (normals * (weight_gain * fan_in ** -0.5)).astype(jnp.bfloat16)


def setup_inputs(seed: int = 0, part: int = 0) -> dict:
    key_list = jax.random.split(jax.random.key(seed), 10)
    patch_vals = jax.random.normal(jax.random.fold_in(key_list[0], part), (BATCH, PATCHES, CHANNELS), jnp.float32)
    ln_base = jnp.array([1.0, 0.0, 1.0, 0.0], jnp.float32)[None, :, None]
    return {
        "x": patch_vals.astype(jnp.bfloat16),
        "w_tok1": normal_weight(key_list[1], (LAYERS, PATCHES, TOKEN_HIDDEN), PATCHES, 1.0),
        "b_tok1": 0.5 * jax.random.normal(key_list[2], (LAYERS, TOKEN_HIDDEN), jnp.float32),
        "w_tok2": normal_weight(key_list[3], (LAYERS, TOKEN_HIDDEN, PATCHES), TOKEN_HIDDEN, 1.5),
        "b_tok2": 0.3 * jax.random.normal(key_list[4], (LAYERS, PATCHES), jnp.float32),
        "w_ch1": normal_weight(key_list[5], (LAYERS, CHANNELS, CHANNEL_HIDDEN), CHANNELS, 1.0),
        "b_ch1": 0.5 * jax.random.normal(key_list[6], (LAYERS, CHANNEL_HIDDEN), jnp.float32),
        "w_ch2": normal_weight(key_list[7], (LAYERS, CHANNEL_HIDDEN, CHANNELS), CHANNEL_HIDDEN, 1.5),
        "b_ch2": 0.3 * jax.random.normal(key_list[8], (LAYERS, CHANNELS), jnp.float32),
        "ln_params": ln_base + 0.3 * jax.random.normal(key_list[9], (LAYERS, 4, CHANNELS), jnp.float32),
    }


def layer_norm(rows_in, ln_scale, ln_offset):
    row_vals = rows_in.astype(jnp.float32)
    row_mean = jnp.mean(row_vals, axis=-1, keepdims=True)
    centered = row_vals - row_mean
    row_var = jnp.mean(centered * centered, axis=-1, keepdims=True)
    return (centered * lax.rsqrt(row_var + LN_EPS) * ln_scale + ln_offset).astype(jnp.bfloat16)


def mixer_layer(act_in, layer_params):
    w_tok1, b_tok1, w_tok2, b_tok2, w_ch1, b_ch1, w_ch2, b_ch2, ln_layer = layer_params
    u_norm = layer_norm(act_in, ln_layer[0], ln_layer[1])
    hidden = jnp.dot(w_tok1.T, u_norm, preferred_element_type=jnp.float32) + b_tok1[:, None]
    g_act = jax.nn.gelu(hidden, approximate=True).astype(jnp.bfloat16)
    t_tok = (jnp.dot(w_tok2.T, g_act, preferred_element_type=jnp.float32) + b_tok2[:, None]).astype(jnp.bfloat16)
    x_mid = (act_in.astype(jnp.float32) + t_tok.astype(jnp.float32)).astype(jnp.bfloat16)
    v_norm = layer_norm(x_mid, ln_layer[2], ln_layer[3])
    pre_act = jnp.dot(v_norm, w_ch1, preferred_element_type=jnp.float32) + b_ch1
    a_act = jax.nn.gelu(pre_act, approximate=True).astype(jnp.bfloat16)
    ch_out = jnp.dot(a_act, w_ch2, preferred_element_type=jnp.float32) + b_ch2
    return (x_mid.astype(jnp.float32) + ch_out).astype(jnp.bfloat16)


def reference(x, w_tok1, b_tok1, w_tok2, b_tok2, w_ch1, b_ch1, w_ch2, b_ch2, ln_params):
    stacked = (w_tok1, b_tok1, w_tok2, b_tok2, w_ch1, b_ch1, w_ch2, b_ch2, ln_params)

    def layer_step(state_in, layer_params):
        return mixer_layer(state_in, layer_params), None

    def one_image(image_in):
        result, _ = lax.scan(layer_step, image_in, stacked)
        return result

    return lax.map(one_image, x)
```

```python
import functools

import jax
import jax.numpy as jnp
from jax import lax
from jax.experimental import pallas as pl
from jax.experimental.pallas import tpu as pltpu
from jax.sharding import PartitionSpec as P

LN_EPS = 1e-6
CHUNKS = 4
GELU_A = 0.7978845608028654
GELU_B = 0.7978845608028654 * 0.044715


def gelu(h):
    return 0.5 * h * (1.0 + jnp.tanh(h * (GELU_A + GELU_B * (h * h))))


def norm(rows, scale, offset):
    mean = jnp.mean(rows, axis=-1, keepdims=True)
    centered = rows - mean
    var = jnp.mean(centered * centered, axis=-1, keepdims=True)
    return (centered * lax.rsqrt(var + LN_EPS) * scale + offset).astype(jnp.bfloat16)


def contract0(a, b):
    return lax.dot_general(a, b, (((0,), (0,)), ((), ())), preferred_element_type=jnp.float32)


def token_in(x, w1_ref, ln_ref):
    u = norm(x.astype(jnp.float32), ln_ref[0:1, :], ln_ref[1:2, :])
    return contract0(w1_ref[...], u)


def first_kernel(x_ref, w1_ref, ln_ref, h_ref):
    h_ref[0] = token_in(x_ref[0], w1_ref, ln_ref)


def channel(x_ref, g_ref, w2_ref, b2_ref, wc1_ref, bc1_ref, wc2_ref, bc2_ref, ln_ref, a_ref):
    t = (contract0(w2_ref[...], g_ref[0]) + b2_ref[...]).astype(jnp.bfloat16)
    x1 = (x_ref[0].astype(jnp.float32) + t.astype(jnp.float32)).astype(jnp.bfloat16)
    v = norm(x1.astype(jnp.float32), ln_ref[2:3, :], ln_ref[3:4, :])
    width = 512
    for e in range(0, wc1_ref.shape[1], width):
        cols = slice(e, e + width)
        pre = jnp.dot(v, wc1_ref[:, cols], preferred_element_type=jnp.float32) + bc1_ref[:, cols]
        a_ref[:, cols] = gelu(pre).astype(jnp.bfloat16)
    out = jnp.dot(a_ref[...], wc2_ref[...], preferred_element_type=jnp.float32) + bc2_ref[...]
    return (x1.astype(jnp.float32) + out).astype(jnp.bfloat16)


def last_kernel(x_ref, g_ref, w2_ref, b2_ref, wc1_ref, bc1_ref, wc2_ref, bc2_ref, ln_ref, z_ref, a_ref):
    z_ref[0] = channel(x_ref, g_ref, w2_ref, b2_ref, wc1_ref, bc1_ref, wc2_ref, bc2_ref, ln_ref, a_ref)


def middle_kernel(x_ref, g_ref, w2_ref, b2_ref, wc1_ref, bc1_ref, wc2_ref, bc2_ref, ln_ref, w1n_ref, lnn_ref, z_ref, h_ref, a_ref):
    z = channel(x_ref, g_ref, w2_ref, b2_ref, wc1_ref, bc1_ref, wc2_ref, bc2_ref, ln_ref, a_ref)
    z_ref[0] = z
    h_ref[0] = token_in(z, w1n_ref, lnn_ref)


def whole(a):
    return pl.BlockSpec(a.shape, lambda i: (0,) * a.ndim)


def image(shape):
    return pl.BlockSpec((1,) + shape, lambda i: (i, 0, 0))


def solution(mesh):
    def local_layers(x, w_tok1, b_tok1, w_tok2, b_tok2, w_ch1, b_ch1, w_ch2, b_ch2, ln_params):
        layers = w_tok1.shape[0]
        batch, rows, chans = x.shape
        hid = w_tok1.shape[2]
        me = lax.axis_index("seq")
        size = batch // CHUNKS
        w1 = lax.dynamic_slice_in_dim(w_tok1, me * rows, rows, 1)
        w2 = lax.dynamic_slice_in_dim(w_tok2, me * rows, rows, 2)
        b2 = lax.dynamic_slice_in_dim(b_tok2, me * rows, rows, 1)[:, :, None]
        own = hid // mesh.shape["seq"]
        b1 = lax.dynamic_slice_in_dim(b_tok1, me * own, own, 1)[:, None, :, None]
        params = pltpu.CompilerParams(vmem_limit_bytes=50 * 1024 * 1024)

        def first(xc):
            return pl.pallas_call(
                first_kernel,
                grid=(size,),
                out_shape=jax.ShapeDtypeStruct((size, hid, chans), jnp.float32),
                in_specs=[image((rows, chans)), whole(w1[0]), whole(ln_params[0])],
                out_specs=image((hid, chans)),
                compiler_params=params,
                cost_estimate=pl.CostEstimate(flops=2 * size * rows * hid * chans, bytes_accessed=size * chans * (2 * rows + 4 * hid), transcendentals=0),
            )(xc, w1[0], ln_params[0])

        def rest(l, xc, g):
            args = [xc, g, w2[l], b2[l], w_ch1[l], b_ch1[l][None], w_ch2[l], b_ch2[l][None], ln_params[l]]
            specs = [image((rows, chans)), image((hid, chans))] + [whole(a) for a in args[2:]]
            outs = [jax.ShapeDtypeStruct((size, rows, chans), jnp.bfloat16)]
            out_specs = [image((rows, chans))]
            body = last_kernel
            if l + 1 < layers:
                body = middle_kernel
                args += [w1[l + 1], ln_params[l + 1]]
                specs += [whole(a) for a in args[-2:]]
                outs.append(jax.ShapeDtypeStruct((size, hid, chans), jnp.float32))
                out_specs.append(image((hid, chans)))
            wide = w_ch1.shape[2]
            return pl.pallas_call(
                body,
                grid=(size,),
                out_shape=outs,
                in_specs=specs,
                out_specs=out_specs,
                scratch_shapes=[pltpu.VMEM((rows, wide), jnp.bfloat16)],
                compiler_params=params,
                cost_estimate=pl.CostEstimate(flops=4 * size * rows * wide * chans, bytes_accessed=4 * size * chans * rows, transcendentals=0),
            )(*args)

        xs = [x[c * size:(c + 1) * size] for c in range(CHUNKS)]
        hs = [first(xc) for xc in xs]
        for l in range(layers):
            gs = []
            for h in hs:
                part = lax.psum_scatter(h, "seq", scatter_dimension=1, tiled=True)
                g = jax.nn.gelu(part + b1[l], approximate=True).astype(jnp.bfloat16)
                gs.append(lax.all_gather(g, "seq", axis=1, tiled=True))
            res = [rest(l, xc, g) for xc, g in zip(xs, gs)]
            xs = [r[0] for r in res]
            hs = [r[1] for r in res if len(r) > 1]
        return jnp.concatenate(xs, 0)

    act = P("data", "seq", None)
    rep = P()
    return jax.shard_map(local_layers, mesh=mesh, in_specs=(act,) + (rep,) * 9, out_specs=act, check_vma=False)
```

```python
import functools

import jax
import jax.numpy as jnp
from jax import lax
from jax.experimental import pallas as pl
from jax.experimental.pallas import tpu as pltpu
from jax.sharding import PartitionSpec as P

F32 = jnp.float32
BF16 = jnp.bfloat16
MESH = pl.DeviceIdType.MESH
LN_EPS = 1e-6
GELU_A = 0.7978845608028654
GELU_B = GELU_A * 0.044715

GROUP = 2
SLOTS = 10
HELD = 4
LAG = 12
WIDTH = 256
STRIP = 32

P1, M1L, M1R, M2L, M2R, GL, GR, GP, FL, FR, PA, PB, PC = range(13)
KINDS = 13


def dot(a, b):
    return jnp.dot(a, b, preferred_element_type=F32)


def gelu(h):
    return 0.5 * h * (1.0 + jnp.tanh(h * (GELU_A + GELU_B * (h * h))))


def gelu_of_half(h):
    return h + h * jnp.tanh(h * (2.0 * GELU_A + (8.0 * GELU_B) * (h * h)))


def norm(rows, scale, offset):
    rows = rows.astype(F32)
    mean = jnp.mean(rows, axis=-1, keepdims=True)
    centered = rows - mean
    var = jnp.mean(centered * centered, axis=-1, keepdims=True)
    return (centered * lax.rsqrt(var + LN_EPS) * scale + offset).astype(BF16)


def kernel(chips, x_hbm, w1, w2, b1, b2, wc1_hbm, bc1, wc2_hbm, bc2, ln, z_hbm,
           xb, wc1, wc2, act, v0, v1, tb, ub, hpart, pbuf, cbuf, m1, m2, gall,
           xsem, wsem, zsem, ssem, rsem):
    batch, rows, chans = x_hbm.shape
    layers = w1.shape[0]
    wide = wc1.shape[2]
    groups = batch // GROUP
    items = layers * groups
    own = gall.shape[3]
    half = own // 2

    me = lax.axis_index("seq")
    chip, core = lax.div(me, 2), lax.rem(me, 2)
    right = lax.rem(chip + 1, chips)
    left = lax.rem(chip + chips - 1, chips)
    far = lax.rem(chip + 2, chips)
    dev_right, dev_left, dev_pair = 2 * right + core, 2 * left + core, 2 * chip + (1 - core)
    mine = core * chips
    other = (1 - core) * chips

    barrier = pltpu.get_barrier_semaphore()
    for dev in (dev_left, dev_right, dev_pair):
        pl.semaphore_signal(barrier, inc=1, device_id={"seq": dev}, device_id_type=MESH)
    pl.semaphore_wait(barrier, 3)

    def load_x(g):
        at = pl.ds(g * GROUP, GROUP)
        return pltpu.make_async_copy(x_hbm.at[at], xb.at[at], xsem.at[g])

    def store_z(g):
        at = pl.ds(g * GROUP, GROUP)
        return pltpu.make_async_copy(xb.at[at], z_hbm.at[at], zsem.at[g])

    def weight_copies():
        return (pltpu.make_async_copy(wc1_hbm, wc1, wsem.at[0]), pltpu.make_async_copy(wc2_hbm, wc2, wsem.at[1]))

    for g in range(groups):
        load_x(g).start()
    for c in weight_copies():
        c.start()

    def remote(kind, slot, dev, src, dst):
        return pltpu.make_async_remote_copy(
            src_ref=src, dst_ref=dst, send_sem=ssem.at[kind, slot], recv_sem=rsem.at[kind, slot],
            device_id={"seq": dev}, device_id_type=MESH)

    def stage(s, lag, fn):
        i = s - lag

        @pl.when((i >= 0) & (i < items))
        def _():
            fn(i, lax.rem(i, SLOTS))

    def wait(kind, slot, dev, region):
        c = remote(kind, slot, dev, region, region)
        c.wait_recv()
        c.wait_send()

    def exchange(s):
        def send_pair(i, sl):
            remote(P1, sl, dev_pair, hpart.at[lax.rem(i, HELD), :, 1 - core], pbuf.at[sl]).start()

        def chip_sum(i, sl):
            wait(P1, sl, dev_pair, pbuf.at[sl])
            for g in range(GROUP):
                cbuf[sl, g] = hpart[lax.rem(i, HELD), g, core] + pbuf[sl, g]
            remote(M1L, sl, dev_right, cbuf.at[sl, :, far, pl.ds(0, half)], m1.at[sl, 0]).start()
            remote(M1R, sl, dev_left, cbuf.at[sl, :, far, pl.ds(half, half)], m1.at[sl, 1]).start()

        def pass_sums(i, sl):
            wait(M1L, sl, dev_right, m1.at[sl, 0])
            wait(M1R, sl, dev_left, m1.at[sl, 1])
            for g in range(GROUP):
                cbuf[sl, g, right, 0:half] = cbuf[sl, g, right, 0:half] + m1[sl, 0, g]
                cbuf[sl, g, left, half:own] = cbuf[sl, g, left, half:own] + m1[sl, 1, g]
            remote(M2L, sl, dev_right, cbuf.at[sl, :, right], m2.at[sl, 0]).start()
            remote(M2R, sl, dev_left, cbuf.at[sl, :, left], m2.at[sl, 1]).start()

        def finish_sums(i, sl):
            wait(M2L, sl, dev_right, m2.at[sl, 0])
            wait(M2R, sl, dev_left, m2.at[sl, 1])
            bias = b1[lax.div(i, groups)]
            for g in range(GROUP):
                h = (cbuf[sl, g, chip] + m2[sl, 0, g]) + m2[sl, 1, g] + bias
                gall[sl, g, mine + chip] = gelu(h).astype(BF16)
            block = gall.at[sl, :, mine + chip]
            remote(GL, sl, dev_right, block, block).start()
            remote(GR, sl, dev_left, block, block).start()
            remote(GP, sl, dev_pair, block, block).start()

        def forward(i, sl):
            from_left, from_right = gall.at[sl, :, mine + left], gall.at[sl, :, mine + right]
            wait(GL, sl, dev_right, from_left)
            wait(GR, sl, dev_left, from_right)
            wait(GP, sl, dev_pair, gall.at[sl, :, other + chip])
            a = gall.at[sl, :, mine + left, pl.ds(0, half)]
            b = gall.at[sl, :, mine + right, pl.ds(half, half)]
            remote(FL, sl, dev_right, a, a).start()
            remote(FR, sl, dev_left, b, b).start()
            remote(PA, sl, dev_pair, from_left, from_left).start()
            remote(PB, sl, dev_pair, from_right, from_right).start()

        def forward_far(i, sl):
            wait(FL, sl, dev_right, gall.at[sl, :, mine + far, pl.ds(0, half)])
            wait(FR, sl, dev_left, gall.at[sl, :, mine + far, pl.ds(half, half)])
            wait(PA, sl, dev_pair, gall.at[sl, :, other + left])
            wait(PB, sl, dev_pair, gall.at[sl, :, other + right])
            block = gall.at[sl, :, mine + far]
            remote(PC, sl, dev_pair, block, block).start()

        def complete(i, sl):
            wait(PC, sl, dev_pair, gall.at[sl, :, other + far])

        stage(s, 1, send_pair)
        stage(s, 2, chip_sum)
        stage(s, 4, pass_sums)
        stage(s, 6, finish_sums)
        stage(s, 8, forward)
        stage(s, 10, forward_far)
        stage(s, 11, complete)

    def unit(s, j, do_a, do_b, do_c, do_h):
        v_cur, v_next = (v0, v1) if j % 2 == 0 else (v1, v0)
        qa = (s - LAG) * GROUP + j
        qb, qc = qa - 1, qa + 1
        if do_a:
            la = lax.div(qa, batch)
        if do_b:
            lb = lax.div(jnp.maximum(qb, 0), batch)
            ib = jnp.where(qb < 0, batch, lax.rem(jnp.maximum(qb, 0), batch))
        if do_c:
            lc = jnp.minimum(lax.div(qc, batch), layers - 1)
            ic = jnp.where(qc >= items * GROUP, batch, lax.rem(qc, batch))
            gc = gall[lax.rem(lax.div(qc, GROUP), SLOTS), lax.rem(qc, GROUP)].reshape(2 * chips * own, chans)
            tb[...] = (dot(w2[lc], gc) + b2[lc]).astype(BF16)
        if do_h:
            lh = lax.div(s, groups)
            ih = lax.rem(s, groups) * GROUP + j
        blocks = wide // WIDTH
        share = rows // blocks
        acc = None
        for k in range(blocks):
            cols = slice(k * WIDTH, (k + 1) * WIDTH)
            if do_b:
                part = dot(act[:, cols], wc2[lb, cols, :])
                acc = part if acc is None else acc + part
            if do_a:
                act[:, cols] = gelu_of_half(dot(v_cur[...], wc1[la, :, cols]) + bc1[la, :, cols]).astype(BF16)
            for r in range(k * share, (k + 1) * share, STRIP):
                strip = slice(r, r + STRIP)
                if do_c:
                    x1 = xb[ic, strip] + tb[strip]
                if do_h:
                    xh = xb[ih, strip]
                if do_c:
                    xb[ic, strip] = x1
                    v_next[strip] = norm(x1, ln[lc, 2:3], ln[lc, 3:4])
                if do_h:
                    ub[strip] = norm(xh, ln[lh, 0:1], ln[lh, 1:2])
        if do_b:
            xb[ib] = (xb[ib].astype(F32) + (acc + bc2[lb])).astype(BF16)
        if do_h:
            hpart[lax.rem(s, HELD), j] = dot(w1[lh], ub[...]).reshape(2, chips, own, chans)

    def finished(s):
        i = s - LAG - 1 - (layers - 1) * groups

        @pl.when((i >= 0) & (i < groups))
        def _():
            store_z(i).start()

    def units(s, *parts):
        for j in range(GROUP):
            unit(s, j, *parts)
            if j == 0 and parts[1]:
                finished(s)

    def step(s, carry):
        exchange(s)

        @pl.when(s < groups)
        def _():
            load_x(s).wait()

        @pl.when(s == LAG // 2)
        def _():
            for c in weight_copies():
                c.wait()

            def scale(r, carry):
                at = pl.ds(pl.multiple_of(r * 64, 64), 64)
                for l in range(layers):
                    wc1[l, at] = wc1[l, at] * jnp.asarray(0.5, BF16)
                return carry

            lax.fori_loop(0, chans // 64, scale, 0)

        @pl.when(s < LAG)
        def _():
            units(s, False, False, False, True)

        @pl.when(s == LAG - 1)
        def _():
            unit(s, GROUP - 1, False, False, True, False)

        @pl.when((s >= LAG) & (s < items))
        def _():
            units(s, True, True, True, True)

        @pl.when((s >= items) & (s < items + LAG))
        def _():
            units(s, True, True, True, False)

        @pl.when(s == items + LAG)
        def _():
            unit(s, 0, False, True, False, False)
            finished(s)

        return carry

    lax.fori_loop(0, items + LAG + 1, step, 0)

    def drain(g, carry):
        store_z(g).wait()
        return carry

    lax.fori_loop(0, groups, drain, 0)


def solution(mesh):
    size = mesh.shape["seq"]
    chips = size // 2

    def local_layers(x, w_tok1, b_tok1, w_tok2, b_tok2, w_ch1, b_ch1, w_ch2, b_ch2, ln_params):
        layers = w_tok1.shape[0]
        batch, rows, chans = x.shape
        hid, wide = w_tok1.shape[2], w_ch1.shape[2]
        own = hid // size
        groups = batch // GROUP
        me = lax.axis_index("seq")
        w1 = lax.dynamic_slice_in_dim(w_tok1, me * rows, rows, 1).transpose(0, 2, 1)
        w2 = lax.dynamic_slice_in_dim(w_tok2, me * rows, rows, 2).transpose(0, 2, 1)
        b2 = lax.dynamic_slice_in_dim(b_tok2, me * rows, rows, 1)[:, :, None]
        first = ((me % 2) * chips + me // 2) * own
        b1 = lax.dynamic_slice_in_dim(b_tok1, first, own, 1)[:, :, None]
        vmem = pl.BlockSpec(memory_space=pltpu.VMEM)
        hbm = pl.BlockSpec(memory_space=pl.ANY)
        tile = pltpu.VMEM((rows, chans), BF16)
        return pl.pallas_call(
            functools.partial(kernel, chips),
            out_shape=jax.ShapeDtypeStruct(x.shape, BF16),
            in_specs=[hbm, vmem, vmem, vmem, vmem, hbm, vmem, hbm, vmem, vmem],
            out_specs=hbm,
            scratch_shapes=[
                pltpu.VMEM((batch + 1, rows, chans), BF16),
                pltpu.VMEM(w_ch1.shape, BF16),
                pltpu.VMEM(w_ch2.shape, BF16),
                pltpu.VMEM((rows, wide), BF16),
                tile, tile, tile, tile,
                pltpu.VMEM((HELD, GROUP, 2, chips, own, chans), F32),
                pltpu.VMEM((SLOTS, GROUP, chips, own, chans), F32),
                pltpu.VMEM((SLOTS, GROUP, chips, own, chans), F32),
                pltpu.VMEM((SLOTS, 2, GROUP, own // 2, chans), F32),
                pltpu.VMEM((SLOTS, 2, GROUP, own, chans), F32),
                pltpu.VMEM((SLOTS, GROUP, 2 * chips, own, chans), BF16),
                pltpu.SemaphoreType.DMA((groups,)),
                pltpu.SemaphoreType.DMA((2,)),
                pltpu.SemaphoreType.DMA((groups,)),
                pltpu.SemaphoreType.DMA((KINDS, SLOTS)),
                pltpu.SemaphoreType.DMA((KINDS, SLOTS)),
            ],
            compiler_params=pltpu.CompilerParams(
                collective_id=0, has_side_effects=True, vmem_limit_bytes=67043328),
        )(x, w1, w2, b1, b2, w_ch1, 0.5 * b_ch1[:, None], w_ch2, b_ch2[:, None], ln_params)

    act = P("data", "seq", None)
    rep = P()
    return jax.shard_map(local_layers, mesh=mesh, in_specs=(act,) + (rep,) * 9, out_specs=act, check_vma=False)
```

```python
import functools

import jax
import jax.numpy as jnp
from jax import lax
from jax.experimental import pallas as pl
from jax.experimental.pallas import tpu as pltpu
from jax.sharding import PartitionSpec as P

F32 = jnp.float32
BF16 = jnp.bfloat16
MESH = pl.DeviceIdType.MESH
LN_EPS = 1e-6
GELU_A = 0.7978845608028654
GELU_B = GELU_A * 0.044715

GROUP = 2
SLOTS = 9
HELD = 2
LAG = 15
WIDTH = 256
STRIP = 32

P1, M1L, M1R, M2L, M2R, GL, GR, GP, FL, FR, PX = range(11)
KINDS = 11
OWN, RIGHT, LEFT, FAR = range(4)
MINE, OTHER = range(2)
LEFT_OVER = 2


def dot(a, b):
    return jnp.dot(a, b, preferred_element_type=F32)


def gelu(h):
    return 0.5 * h * (1.0 + jnp.tanh(h * (GELU_A + GELU_B * (h * h))))


def gelu_of_half(h):
    return h + h * jnp.tanh(h * (2.0 * GELU_A + (8.0 * GELU_B) * (h * h)))


def norm(rows, scale, offset):
    rows = rows.astype(F32)
    mean = jnp.mean(rows, axis=-1, keepdims=True)
    centered = rows - mean
    var = jnp.mean(centered * centered, axis=-1, keepdims=True)
    return (centered * lax.rsqrt(var + LN_EPS) * scale + offset).astype(BF16)


def column(row, offset, count):
    shape = (count, row.shape[1])
    hit = lax.broadcasted_iota(jnp.int32, shape, 1) == lax.broadcasted_iota(jnp.int32, shape, 0) + offset
    return jnp.sum(jnp.where(hit, row, 0.0), axis=1, keepdims=True)


def kernel(chips, x_hbm, w1_hbm, b1_row, w2_hbm, b2_row, wc1_hbm, bc1, wc2_hbm, bc2, ln, z_hbm,
           xb, wc1, wc2, act, v0, v1, tb, ub, hpart, pbuf, cbuf, m1, m2, gall, w1_raw, w2_raw, w1, w2, b1, b2,
           xsem, wsem, zsem, ssem, rsem):
    batch, rows, chans = x_hbm.shape
    layers = w1.shape[0]
    wide = wc1.shape[2]
    groups = batch // GROUP
    items = layers * groups
    last = items - LEFT_OVER
    stop = last * GROUP + LAG
    own = gall.shape[4]
    half = own // 2

    me = lax.axis_index("seq")
    chip, core = lax.div(me, 2), lax.rem(me, 2)
    right = lax.rem(chip + 1, chips)
    left = lax.rem(chip + chips - 1, chips)
    far = lax.rem(chip + 2, chips)
    dev_right, dev_left, dev_pair = 2 * right + core, 2 * left + core, 2 * chip + (1 - core)
    order = [(c * chips + k) * own for c in (core, 1 - core) for k in (chip, right, left, far)]

    def load_x(g):
        at = pl.ds(g * GROUP, GROUP)
        return pltpu.make_async_copy(x_hbm.at[at], xb.at[at], xsem.at[g])

    def store_z(g):
        at = pl.ds(g * GROUP, GROUP)
        return pltpu.make_async_copy(xb.at[at], z_hbm.at[at], zsem.at[g])

    def weight_copies():
        return (pltpu.make_async_copy(wc1_hbm, wc1, wsem.at[0]), pltpu.make_async_copy(wc2_hbm, wc2, wsem.at[1]))

    mixing_rows = pl.ds(pl.multiple_of(me * rows, rows), rows)
    rest = pl.ds(1, layers - 1)
    mixing = (pltpu.make_async_copy(w1_hbm.at[0, mixing_rows], w1_raw.at[0], wsem.at[2]),
              pltpu.make_async_copy(w1_hbm.at[rest, mixing_rows], w1_raw.at[rest], wsem.at[3]),
              pltpu.make_async_copy(w2_hbm.at[:, :, mixing_rows], w2_raw, wsem.at[4]))

    barrier = pltpu.get_barrier_semaphore()
    for dev in (dev_left, dev_right, dev_pair):
        pl.semaphore_signal(barrier, inc=1, device_id={"seq": dev}, device_id_type=MESH)
    mixing[0].start()
    load_x(0).start()

    hid = 2 * chips * own

    def place_w1(l):
        ub[0:hid] = w1_raw[l].T
        for n, at in enumerate(order):
            w1[l, n * own:(n + 1) * own] = ub[pl.ds(pl.multiple_of(at, own), own)]

    def place_rest():
        for l in range(1, layers):
            place_w1(l)
        for l in range(layers):
            for n, at in enumerate(order):
                tb[n * own:(n + 1) * own] = w2_raw[l, pl.ds(pl.multiple_of(at, own), own)]
            w2[l] = tb[0:hid].T
            b1[l] = column(b1_row[l:l + 1], order[0], own)
            for r in range(0, rows, 128):
                at = pl.ds(pl.multiple_of(me * rows + r, 128), 128)
                b2[l, r:r + 128] = column(b2_row[l:l + 1, at], 0, 128)

    mixing[0].wait()
    place_w1(0)
    for g in range(1, groups):
        load_x(g).start()
    for c in mixing[1:] + weight_copies():
        c.start()
    pl.semaphore_wait(barrier, 3)

    def remote(kind, slot, dev, src, dst):
        return pltpu.make_async_remote_copy(
            src_ref=src, dst_ref=dst, send_sem=ssem.at[kind, slot], recv_sem=rsem.at[kind, slot],
            device_id={"seq": dev}, device_id_type=MESH)

    def stage(s, lag, fn):
        i = s - lag

        @pl.when((i >= 0) & (i < items))
        def _():
            fn(i, lax.rem(i, SLOTS))

    def wait(kind, slot, dev, region):
        c = remote(kind, slot, dev, region, region)
        c.wait_recv()
        c.wait_send()

    def exchange(s, point):
        def send_pair(i, sl):
            remote(P1, sl, dev_pair, hpart.at[lax.rem(i, HELD), :, OTHER], pbuf.at[sl]).start()

        def chip_sum(i, sl):
            wait(P1, sl, dev_pair, pbuf.at[sl])
            for g in range(GROUP):
                cbuf[sl, g] = hpart[lax.rem(i, HELD), g, MINE] + pbuf[sl, g]
            remote(M1L, sl, dev_right, cbuf.at[sl, :, FAR, pl.ds(0, half)], m1.at[sl, 0]).start()
            remote(M1R, sl, dev_left, cbuf.at[sl, :, FAR, pl.ds(half, half)], m1.at[sl, 1]).start()

        def pass_sums(i, sl):
            wait(M1L, sl, dev_right, m1.at[sl, 0])
            wait(M1R, sl, dev_left, m1.at[sl, 1])
            for g in range(GROUP):
                cbuf[sl, g, RIGHT, 0:half] = cbuf[sl, g, RIGHT, 0:half] + m1[sl, 0, g]
                cbuf[sl, g, LEFT, half:own] = cbuf[sl, g, LEFT, half:own] + m1[sl, 1, g]
            remote(M2L, sl, dev_right, cbuf.at[sl, :, RIGHT], m2.at[sl, 0]).start()
            remote(M2R, sl, dev_left, cbuf.at[sl, :, LEFT], m2.at[sl, 1]).start()

        def finish_sums(i, sl):
            wait(M2L, sl, dev_right, m2.at[sl, 0])
            wait(M2R, sl, dev_left, m2.at[sl, 1])
            bias = b1[lax.div(i, groups)]
            for g in range(GROUP):
                h = (cbuf[sl, g, OWN] + m2[sl, 0, g]) + m2[sl, 1, g] + bias
                gall[sl, g, MINE, OWN] = gelu(h).astype(BF16)
            block = gall.at[sl, :, MINE, OWN]
            remote(GL, sl, dev_right, block, gall.at[sl, :, MINE, LEFT]).start()
            remote(GR, sl, dev_left, block, gall.at[sl, :, MINE, RIGHT]).start()
            remote(GP, sl, dev_pair, block, gall.at[sl, :, OTHER, OWN]).start()

        def forward(i, sl):
            wait(GL, sl, dev_right, gall.at[sl, :, MINE, LEFT])
            wait(GR, sl, dev_left, gall.at[sl, :, MINE, RIGHT])
            wait(GP, sl, dev_pair, gall.at[sl, :, OTHER, OWN])
            a, b = pl.ds(0, half), pl.ds(half, half)
            remote(FL, sl, dev_right, gall.at[sl, :, MINE, LEFT, a], gall.at[sl, :, MINE, FAR, a]).start()
            remote(FR, sl, dev_left, gall.at[sl, :, MINE, RIGHT, b], gall.at[sl, :, MINE, FAR, b]).start()

        def forward_far(i, sl):
            wait(FL, sl, dev_right, gall.at[sl, :, MINE, FAR, pl.ds(0, half)])
            wait(FR, sl, dev_left, gall.at[sl, :, MINE, FAR, pl.ds(half, half)])
            rest = pl.ds(RIGHT, chips - 1)
            remote(PX, sl, dev_pair, gall.at[sl, :, MINE, rest], gall.at[sl, :, OTHER, rest]).start()

        def complete(i, sl):
            wait(PX, sl, dev_pair, gall.at[sl, :, OTHER, pl.ds(RIGHT, chips - 1)])

        if point == 0:
            stage(s, 1, send_pair)
            stage(s, 3, pass_sums)
            stage(s, 4, finish_sums)
            stage(s, 7, complete)
        else:
            stage(s, 1, chip_sum)
            stage(s, 5, forward)
            stage(s, 6, forward_far)

    def unit(s, j, do_a, do_b, do_c, do_h):
        v_cur, v_next = (v0, v1) if (j + LAG) % 2 == 0 else (v1, v0)
        qa = s * GROUP + j - LAG
        qb, qc = qa - 1, qa + 1
        if do_a:
            la = lax.div(qa, batch)
        if do_b:
            lb = lax.div(jnp.maximum(qb, 0), batch)
            ib = jnp.where(qb < 0, batch, lax.rem(jnp.maximum(qb, 0), batch))
        if do_c:
            lc = jnp.minimum(lax.div(qc, batch), layers - 1)
            ic = jnp.where(qc >= items * GROUP, batch, lax.rem(qc, batch))
            gc = gall[lax.rem(lax.div(qc, GROUP), SLOTS), lax.rem(qc, GROUP)].reshape(2 * chips * own, chans)
            tb[...] = (dot(w2[lc], gc) + b2[lc]).astype(BF16)
        if do_h:
            lh = lax.div(s, groups)
            ih = lax.rem(s, groups) * GROUP + j
        blocks = wide // WIDTH
        share = rows // blocks
        acc = None
        for k in range(blocks):
            cols = slice(k * WIDTH, (k + 1) * WIDTH)
            if do_b:
                part = dot(act[:, cols], wc2[lb, cols, :])
                acc = part if acc is None else acc + part
            if do_a:
                act[:, cols] = gelu_of_half(dot(v_cur[...], wc1[la, :, cols]) + 0.5 * bc1[pl.ds(la, 1), cols]).astype(BF16)
            for r in range(k * share, (k + 1) * share, STRIP):
                strip = slice(r, r + STRIP)
                if do_c:
                    x1 = xb[ic, strip] + tb[strip]
                if do_h:
                    xh = xb[ih, strip]
                if do_c:
                    xb[ic, strip] = x1
                    v_next[strip] = norm(x1, ln[lc, 2:3], ln[lc, 3:4])
                if do_h:
                    ub[strip] = norm(xh, ln[lh, 0:1], ln[lh, 1:2])
        if do_b:
            xb[ib] = (xb[ib].astype(F32) + (acc + bc2[pl.ds(lb, 1), :])).astype(BF16)
        if do_h:
            hpart[lax.rem(s, HELD), j] = dot(w1[lh], ub[...]).reshape(2, chips, own, chans)

    def finished(s, j):
        before = items - groups
        i = s + (j - LAG) // GROUP

        @pl.when((i - 1 >= before) & (i - 1 < last))
        def _():
            store_z(i - 1 - before).start()

        @pl.when((i >= last) & (i < items))
        def _():
            store_z(i - before).start()

    def step(s, carry):
        @pl.when(s < groups)
        def _():
            load_x(s).wait()

        @pl.when(s == 1)
        def _():
            for c in mixing[1:]:
                c.wait()
            place_rest()

        @pl.when(s == 3)
        def _():
            for c in weight_copies():
                c.wait()

            def scale(r, carry):
                at = pl.ds(pl.multiple_of(r * 64, 64), 64)
                for l in range(layers):
                    wc1[l, at] = wc1[l, at] * jnp.asarray(0.5, BF16)
                return carry

            lax.fori_loop(0, chans // 64, scale, 0)

        for j in range(GROUP):
            exchange(s, j)

            n = s * GROUP + j

            @pl.when(n < LAG)
            def _():
                unit(s, j, False, False, False, True)

            @pl.when((n >= LAG) & (s < items))
            def _():
                unit(s, j, True, True, True, True)

            @pl.when((s >= items) & (n < stop))
            def _():
                unit(s, j, True, True, True, False)

            only_c = (n > stop) & (n < items * GROUP + LAG - 1)
            if (j + LAG) % GROUP == 0:
                @pl.when(n == stop)
                def _():
                    unit(s, j, False, True, True, False)
            else:
                only_c = only_c | (n == LAG - 1)

            @pl.when(only_c)
            def _():
                unit(s, j, False, False, True, False)

            if (j + LAG) % GROUP == 0:
                finished(s, j)

        return carry

    lax.fori_loop(0, items + LAG // GROUP, step, 0)

    def drain(g, carry):
        store_z(g).wait()
        return carry

    lax.fori_loop(0, groups, drain, 0)


def last_kernel(x_hbm, wc1_hbm, bc1, wc2_hbm, bc2, ln, z_hbm, xb, wc1, wc2, act, v0, v1, xsem, wsem, zsem):
    batch, rows, chans = x_hbm.shape
    layer = wc1_hbm.shape[0] - 1
    wide = wc1.shape[1]
    groups = batch // GROUP
    first = groups - LEFT_OVER
    pace = pl.cdiv(first, LEFT_OVER)

    def load(g):
        at = pl.ds(g * GROUP, GROUP)
        return pltpu.make_async_copy(x_hbm.at[at], xb.at[at], xsem.at[g])

    def store(g):
        at = pl.ds(g * GROUP, GROUP)
        return pltpu.make_async_copy(xb.at[at], z_hbm.at[at], zsem.at[g])

    weights = (pltpu.make_async_copy(wc1_hbm.at[layer], wc1, wsem.at[0]),
               pltpu.make_async_copy(wc2_hbm.at[layer], wc2, wsem.at[1]))
    load(first).start()
    for c in weights:
        c.start()
    for g in range(first + 1, groups):
        load(g).start()

    def prepare(v, i, strip):
        v[strip] = norm(xb[i, strip], ln[layer, 2:3], ln[layer, 3:4])

    def unit(i, v_cur, v_next, do_a):
        blocks = wide // WIDTH
        share = rows // blocks
        acc = None
        before = jnp.maximum(i - 1, first * GROUP)
        after = jnp.minimum(i + 1, batch - 1)
        for k in range(blocks):
            cols = slice(k * WIDTH, (k + 1) * WIDTH)
            part = dot(act[:, cols], wc2[cols])
            acc = part if acc is None else acc + part
            if do_a:
                pre = dot(v_cur[...], wc1[:, cols]) + 0.5 * bc1[layer:layer + 1, cols]
                act[:, cols] = gelu_of_half(pre).astype(BF16)
                for r in range(k * share, (k + 1) * share, STRIP):
                    prepare(v_next, after, slice(r, r + STRIP))
        z = (xb[before].astype(F32) + (acc + bc2[layer:layer + 1])).astype(BF16)
        return before, z

    load(first).wait()
    for r in range(0, rows, STRIP):
        prepare(v0, first * GROUP, slice(r, r + STRIP))
    for c in weights:
        c.wait()

    def scale(r, carry):
        at = pl.ds(pl.multiple_of(r * 64, 64), 64)
        wc1[at] = wc1[at] * jnp.asarray(0.5, BF16)
        return carry

    lax.fori_loop(0, chans // 64, scale, 0)
    for g in range(first):
        load(g).start()

    def pair(p, carry):
        g = first + p

        @pl.when(g + 1 < groups)
        def _():
            load(jnp.minimum(g + 1, groups - 1)).wait()

        before, z = unit(g * GROUP, v0, v1, True)

        @pl.when(p > 0)
        def _():
            xb[before] = z
            store(jnp.maximum(g - 1, first)).start()

        before, z = unit(g * GROUP + 1, v1, v0, True)
        xb[before] = z
        for n in range(pace):
            other = p * pace + n

            @pl.when(other < first)
            def _():
                load(jnp.minimum(other, first - 1)).wait()
                store(jnp.minimum(other, first - 1)).start()

        return carry

    lax.fori_loop(0, LEFT_OVER, pair, 0)
    before, z = unit(batch, v0, v1, False)
    xb[before] = z
    store(groups - 1).start()

    def drain(g, carry):
        store(g).wait()
        return carry

    lax.fori_loop(0, groups, drain, 0)


def solution(mesh):
    size = mesh.shape["seq"]
    chips = size // 2

    def local_layers(x, w_tok1, b_tok1, w_tok2, b_tok2, w_ch1, b_ch1, w_ch2, b_ch2, ln_params):
        layers = w_tok1.shape[0]
        batch, rows, chans = x.shape
        hid, wide = w_tok1.shape[2], w_ch1.shape[2]
        own = hid // size
        groups = batch // GROUP
        vmem = pl.BlockSpec(memory_space=pltpu.VMEM)
        hbm = pl.BlockSpec(memory_space=pl.ANY)
        tile = pltpu.VMEM((rows, chans), BF16)
        most = pl.pallas_call(
            functools.partial(kernel, chips),
            out_shape=jax.ShapeDtypeStruct(x.shape, BF16),
            in_specs=[hbm, hbm, vmem, hbm, vmem, hbm, vmem, hbm, vmem, vmem],
            out_specs=hbm,
            scratch_shapes=[
                pltpu.VMEM((batch + 1, rows, chans), BF16),
                pltpu.VMEM(w_ch1.shape, BF16),
                pltpu.VMEM(w_ch2.shape, BF16),
                pltpu.VMEM((rows, wide), BF16),
                tile, tile, tile, tile,
                pltpu.VMEM((HELD, GROUP, 2, chips, own, chans), F32),
                pltpu.VMEM((SLOTS, GROUP, chips, own, chans), F32),
                pltpu.VMEM((SLOTS, GROUP, chips, own, chans), F32),
                pltpu.VMEM((SLOTS, 2, GROUP, own // 2, chans), F32),
                pltpu.VMEM((SLOTS, 2, GROUP, own, chans), F32),
                pltpu.VMEM((SLOTS, GROUP, 2, chips, own, chans), BF16),
                pltpu.VMEM((layers, rows, hid), BF16),
                pltpu.VMEM((layers, hid, rows), BF16),
                pltpu.VMEM((layers, hid, rows), BF16),
                pltpu.VMEM((layers, rows, hid), BF16),
                pltpu.VMEM((layers, own, 1), F32),
                pltpu.VMEM((layers, rows, 1), F32),
                pltpu.SemaphoreType.DMA((groups,)),
                pltpu.SemaphoreType.DMA((5,)),
                pltpu.SemaphoreType.DMA((groups,)),
                pltpu.SemaphoreType.DMA((KINDS, SLOTS)),
                pltpu.SemaphoreType.DMA((KINDS, SLOTS)),
            ],
            compiler_params=pltpu.CompilerParams(
                collective_id=0, has_side_effects=True, vmem_limit_bytes=67043328),
        )(x, w_tok1, b_tok1, w_tok2, b_tok2, w_ch1, b_ch1, w_ch2, b_ch2, ln_params)
        return pl.pallas_call(
            last_kernel,
            out_shape=jax.ShapeDtypeStruct(x.shape, BF16),
            in_specs=[hbm, hbm, vmem, hbm, vmem, vmem],
            out_specs=hbm,
            scratch_shapes=[
                pltpu.VMEM(x.shape, BF16),
                pltpu.VMEM(w_ch1.shape[1:], BF16),
                pltpu.VMEM(w_ch2.shape[1:], BF16),
                pltpu.VMEM((rows, wide), BF16),
                tile, tile,
                pltpu.SemaphoreType.DMA((groups,)),
                pltpu.SemaphoreType.DMA((2,)),
                pltpu.SemaphoreType.DMA((groups,)),
            ],
            compiler_params=pltpu.CompilerParams(vmem_limit_bytes=67043328),
        )(most, w_ch1, b_ch1, w_ch2, b_ch2, ln_params)

    act = P("data", "seq", None)
    rep = P()
    return jax.shard_map(local_layers, mesh=mesh, in_specs=(act,) + (rep,) * 9, out_specs=act, check_vma=False)
```

```python
import functools

import jax
import jax.numpy as jnp
from jax import lax
from jax.experimental import pallas as pl
from jax.experimental.pallas import tpu as pltpu
from jax.sharding import PartitionSpec as P

F32 = jnp.float32
BF16 = jnp.bfloat16
MESH = pl.DeviceIdType.MESH
LN_EPS = 1e-6
GELU_A = 0.7978845608028654
GELU_B = GELU_A * 0.044715

GROUP = 2
SLOTS = 9
HELD = 2
LAG = 15
WIDTH = 256
STRIP = 32

P1, M1L, M1R, M2L, M2R, GL, GR, GP, FL, FR, PX = range(11)
KINDS = 11
OWN, RIGHT, LEFT, FAR = range(4)
MINE, OTHER = range(2)
LEFT_OVER = 2


def dot(a, b):
    return jnp.dot(a, b, preferred_element_type=F32)


def gelu(h):
    return 0.5 * h * (1.0 + jnp.tanh(h * (GELU_A + GELU_B * (h * h))))


def gelu_of_half(h):
    return h + h * jnp.tanh(h * (2.0 * GELU_A + (8.0 * GELU_B) * (h * h)))


def norm(rows, scale, offset):
    rows = rows.astype(F32)
    mean = jnp.mean(rows, axis=-1, keepdims=True)
    centered = rows - mean
    var = jnp.mean(centered * centered, axis=-1, keepdims=True)
    return (centered * lax.rsqrt(var + LN_EPS) * scale + offset).astype(BF16)


def column(row, offset, count):
    shape = (count, row.shape[1])
    hit = lax.broadcasted_iota(jnp.int32, shape, 1) == lax.broadcasted_iota(jnp.int32, shape, 0) + offset
    return jnp.sum(jnp.where(hit, row, 0.0), axis=1, keepdims=True)


def kernel(chips, x_hbm, w1_hbm, b1_row, w2_hbm, b2_row, wc1_hbm, bc1, wc2_hbm, bc2, ln, z_hbm,
           xb, wc1, wc2, act, v0, v1, tb, ub, hpart, pbuf, cbuf, m1, m2, gall, w1_raw, w2_raw, w1, w2, b1, b2,
           xsem, wsem, zsem, ssem, rsem):
    batch, rows, chans = x_hbm.shape
    layers = w1.shape[0]
    wide = wc1.shape[2]
    groups = batch // GROUP
    items = layers * groups
    last = items - LEFT_OVER
    stop = last * GROUP + LAG
    own = gall.shape[4]
    half = own // 2

    me = lax.axis_index("seq")
    chip, core = lax.div(me, 2), lax.rem(me, 2)
    right = lax.rem(chip + 1, chips)
    left = lax.rem(chip + chips - 1, chips)
    far = lax.rem(chip + 2, chips)
    dev_right, dev_left, dev_pair = 2 * right + core, 2 * left + core, 2 * chip + (1 - core)
    order = [(c * chips + k) * own for c in (core, 1 - core) for k in (chip, right, left, far)]

    def load_x(g):
        at = pl.ds(g * GROUP, GROUP)
        return pltpu.make_async_copy(x_hbm.at[at], xb.at[at], xsem.at[g])

    def store_z(g):
        at = pl.ds(g * GROUP, GROUP)
        return pltpu.make_async_copy(xb.at[at], z_hbm.at[at], zsem.at[g])

    def weight_copies():
        return (pltpu.make_async_copy(wc1_hbm, wc1, wsem.at[0]), pltpu.make_async_copy(wc2_hbm, wc2, wsem.at[1]))

    mixing_rows = pl.ds(pl.multiple_of(me * rows, rows), rows)
    rest = pl.ds(1, layers - 1)
    mixing = (pltpu.make_async_copy(w1_hbm.at[0, mixing_rows], w1_raw.at[0], wsem.at[2]),
              pltpu.make_async_copy(w1_hbm.at[rest, mixing_rows], w1_raw.at[rest], wsem.at[3]),
              pltpu.make_async_copy(w2_hbm.at[:, :, mixing_rows], w2_raw, wsem.at[4]))

    barrier = pltpu.get_barrier_semaphore()
    for dev in (dev_left, dev_right, dev_pair):
        pl.semaphore_signal(barrier, inc=1, device_id={"seq": dev}, device_id_type=MESH)
    mixing[0].start()
    load_x(0).start()

    hid = 2 * chips * own

    def place_w1(l):
        ub[0:hid] = w1_raw[l].T
        for n, at in enumerate(order):
            w1[l, n * own:(n + 1) * own] = ub[pl.ds(pl.multiple_of(at, own), own)]

    def place_rest():
        for l in range(1, layers):
            place_w1(l)
        for l in range(layers):
            for n, at in enumerate(order):
                tb[n * own:(n + 1) * own] = w2_raw[l, pl.ds(pl.multiple_of(at, own), own)]
            w2[l] = tb[0:hid].T
            b1[l] = column(b1_row[l:l + 1], order[0], own)
            for r in range(0, rows, 128):
                at = pl.ds(pl.multiple_of(me * rows + r, 128), 128)
                b2[l, r:r + 128] = column(b2_row[l:l + 1, at], 0, 128)

    mixing[0].wait()
    place_w1(0)
    for g in range(1, groups):
        load_x(g).start()
    for c in mixing[1:] + weight_copies():
        c.start()
    pl.semaphore_wait(barrier, 3)

    def remote(kind, slot, dev, src, dst):
        return pltpu.make_async_remote_copy(
            src_ref=src, dst_ref=dst, send_sem=ssem.at[kind, slot], recv_sem=rsem.at[kind, slot],
            device_id={"seq": dev}, device_id_type=MESH)

    def stage(s, lag, fn):
        i = s - lag

        @pl.when((i >= 0) & (i < items))
        def _():
            fn(i, lax.rem(i, SLOTS))

    def wait(kind, slot, dev, region):
        c = remote(kind, slot, dev, region, region)
        c.wait_recv()
        c.wait_send()

    def exchange(s, point):
        def send_pair(i, sl):
            remote(P1, sl, dev_pair, hpart.at[lax.rem(i, HELD), :, OTHER], pbuf.at[sl]).start()

        def chip_sum(i, sl):
            wait(P1, sl, dev_pair, pbuf.at[sl])
            for g in range(GROUP):
                cbuf[sl, g] = hpart[lax.rem(i, HELD), g, MINE] + pbuf[sl, g]
            remote(M1L, sl, dev_right, cbuf.at[sl, :, FAR, pl.ds(0, half)], m1.at[sl, 0]).start()
            remote(M1R, sl, dev_left, cbuf.at[sl, :, FAR, pl.ds(half, half)], m1.at[sl, 1]).start()

        def pass_sums(i, sl):
            wait(M1L, sl, dev_right, m1.at[sl, 0])
            wait(M1R, sl, dev_left, m1.at[sl, 1])
            for g in range(GROUP):
                cbuf[sl, g, RIGHT, 0:half] = cbuf[sl, g, RIGHT, 0:half] + m1[sl, 0, g]
                cbuf[sl, g, LEFT, half:own] = cbuf[sl, g, LEFT, half:own] + m1[sl, 1, g]
            remote(M2L, sl, dev_right, cbuf.at[sl, :, RIGHT], m2.at[sl, 0]).start()
            remote(M2R, sl, dev_left, cbuf.at[sl, :, LEFT], m2.at[sl, 1]).start()

        def finish_sums(i, sl):
            wait(M2L, sl, dev_right, m2.at[sl, 0])
            wait(M2R, sl, dev_left, m2.at[sl, 1])
            bias = b1[lax.div(i, groups)]
            for g in range(GROUP):
                h = (cbuf[sl, g, OWN] + m2[sl, 0, g]) + m2[sl, 1, g] + bias
                gall[sl, g, MINE, OWN] = gelu(h).astype(BF16)
            block = gall.at[sl, :, MINE, OWN]
            remote(GL, sl, dev_right, block, gall.at[sl, :, MINE, LEFT]).start()
            remote(GR, sl, dev_left, block, gall.at[sl, :, MINE, RIGHT]).start()
            remote(GP, sl, dev_pair, block, gall.at[sl, :, OTHER, OWN]).start()

        def forward(i, sl):
            wait(GL, sl, dev_right, gall.at[sl, :, MINE, LEFT])
            wait(GR, sl, dev_left, gall.at[sl, :, MINE, RIGHT])
            wait(GP, sl, dev_pair, gall.at[sl, :, OTHER, OWN])
            a, b = pl.ds(0, half), pl.ds(half, half)
            remote(FL, sl, dev_right, gall.at[sl, :, MINE, LEFT, a], gall.at[sl, :, MINE, FAR, a]).start()
            remote(FR, sl, dev_left, gall.at[sl, :, MINE, RIGHT, b], gall.at[sl, :, MINE, FAR, b]).start()

        def forward_far(i, sl):
            wait(FL, sl, dev_right, gall.at[sl, :, MINE, FAR, pl.ds(0, half)])
            wait(FR, sl, dev_left, gall.at[sl, :, MINE, FAR, pl.ds(half, half)])
            rest = pl.ds(RIGHT, chips - 1)
            remote(PX, sl, dev_pair, gall.at[sl, :, MINE, rest], gall.at[sl, :, OTHER, rest]).start()

        def complete(i, sl):
            wait(PX, sl, dev_pair, gall.at[sl, :, OTHER, pl.ds(RIGHT, chips - 1)])

        if point == 0:
            stage(s, 1, send_pair)
            stage(s, 3, pass_sums)
            stage(s, 4, finish_sums)
            stage(s, 7, complete)
        else:
            stage(s, 1, chip_sum)
            stage(s, 5, forward)
            stage(s, 6, forward_far)

    def unit(s, j, do_a, do_b, do_c, do_h):
        v_cur, v_next = (v0, v1) if (j + LAG) % 2 == 0 else (v1, v0)
        qa = s * GROUP + j - LAG
        qb, qc = qa - 1, qa + 1
        if do_a:
            la = lax.div(qa, batch)
        if do_b:
            lb = lax.div(jnp.maximum(qb, 0), batch)
            ib = jnp.where(qb < 0, batch, lax.rem(jnp.maximum(qb, 0), batch))
        if do_c:
            lc = jnp.minimum(lax.div(qc, batch), layers - 1)
            ic = jnp.where(qc >= items * GROUP, batch, lax.rem(qc, batch))
            gc = gall[lax.rem(lax.div(qc, GROUP), SLOTS), lax.rem(qc, GROUP)].reshape(2 * chips * own, chans)
        if do_h:
            lh = lax.div(s, groups)
            ih = lax.rem(s, groups) * GROUP + j
        blocks = wide // WIDTH
        share = rows // blocks
        acc = None
        for k in range(blocks):
            cols = slice(k * WIDTH, (k + 1) * WIDTH)
            if do_c and k % (blocks // 2) == 0:
                part_rows = slice(k * share, (k + blocks // 2) * share)
                tb[part_rows] = (dot(w2[lc, part_rows], gc) + b2[lc, part_rows]).astype(BF16)
            if do_b:
                part = dot(act[:, cols], wc2[lb, cols, :])
                acc = part if acc is None else acc + part
            if do_a:
                act[:, cols] = gelu_of_half(dot(v_cur[...], wc1[la, :, cols]) + 0.5 * bc1[pl.ds(la, 1), cols]).astype(BF16)
            for r in range(k * share, (k + 1) * share, STRIP):
                strip = slice(r, r + STRIP)
                if do_c:
                    x1 = xb[ic, strip] + tb[strip]
                if do_h:
                    xh = xb[ih, strip]
                if do_c:
                    xb[ic, strip] = x1
                    v_next[strip] = norm(x1, ln[lc, 2:3], ln[lc, 3:4])
                if do_h:
                    ub[strip] = norm(xh, ln[lh, 0:1], ln[lh, 1:2])
        if do_b:
            xb[ib] = (xb[ib].astype(F32) + (acc + bc2[pl.ds(lb, 1), :])).astype(BF16)
        if do_h:
            hpart[lax.rem(s, HELD), j] = dot(w1[lh], ub[...]).reshape(2, chips, own, chans)

    def finished(s, j):
        before = items - groups
        i = s + (j - LAG) // GROUP

        @pl.when((i - 1 >= before) & (i - 1 < last))
        def _():
            store_z(i - 1 - before).start()

        @pl.when((i >= last) & (i < items))
        def _():
            store_z(i - before).start()

    def step(s, carry):
        @pl.when(s < groups)
        def _():
            load_x(s).wait()

        @pl.when(s == 1)
        def _():
            for c in mixing[1:]:
                c.wait()
            place_rest()

        @pl.when(s == 3)
        def _():
            for c in weight_copies():
                c.wait()

            def scale(r, carry):
                at = pl.ds(pl.multiple_of(r * 64, 64), 64)
                for l in range(layers):
                    wc1[l, at] = wc1[l, at] * jnp.asarray(0.5, BF16)
                return carry

            lax.fori_loop(0, chans // 64, scale, 0)

        for j in range(GROUP):
            exchange(s, j)

            n = s * GROUP + j

            @pl.when(n < LAG)
            def _():
                unit(s, j, False, False, False, True)

            @pl.when((n >= LAG) & (s < items))
            def _():
                unit(s, j, True, True, True, True)

            @pl.when((s >= items) & (n < stop))
            def _():
                unit(s, j, True, True, True, False)

            only_c = (n > stop) & (n < items * GROUP + LAG - 1)
            if (j + LAG) % GROUP == 0:
                @pl.when(n == stop)
                def _():
                    unit(s, j, False, True, True, False)
            else:
                only_c = only_c | (n == LAG - 1)

            @pl.when(only_c)
            def _():
                unit(s, j, False, False, True, False)

            if (j + LAG) % GROUP == 0:
                finished(s, j)

        return carry

    lax.fori_loop(0, items + LAG // GROUP, step, 0)

    def drain(g, carry):
        store_z(g).wait()
        return carry

    lax.fori_loop(0, groups, drain, 0)


def last_kernel(x_hbm, wc1_hbm, bc1, wc2_hbm, bc2, ln, z_hbm, xb, wc1, wc2, act, v0, v1, xsem, wsem, zsem):
    batch, rows, chans = x_hbm.shape
    layer = wc1_hbm.shape[0] - 1
    wide = wc1.shape[1]
    groups = batch // GROUP
    first = groups - LEFT_OVER
    pace = pl.cdiv(first, LEFT_OVER)

    def load(g):
        at = pl.ds(g * GROUP, GROUP)
        return pltpu.make_async_copy(x_hbm.at[at], xb.at[at], xsem.at[g])

    def store(g):
        at = pl.ds(g * GROUP, GROUP)
        return pltpu.make_async_copy(xb.at[at], z_hbm.at[at], zsem.at[g])

    weights = (pltpu.make_async_copy(wc1_hbm.at[layer], wc1, wsem.at[0]),
               pltpu.make_async_copy(wc2_hbm.at[layer], wc2, wsem.at[1]))
    load(first).start()
    for c in weights:
        c.start()
    for g in range(first + 1, groups):
        load(g).start()

    def prepare(v, i, strip):
        v[strip] = norm(xb[i, strip], ln[layer, 2:3], ln[layer, 3:4])

    def unit(i, v_cur, v_next, do_a):
        blocks = wide // WIDTH
        share = rows // blocks
        acc = None
        before = jnp.maximum(i - 1, first * GROUP)
        after = jnp.minimum(i + 1, batch - 1)
        for k in range(blocks):
            cols = slice(k * WIDTH, (k + 1) * WIDTH)
            part = dot(act[:, cols], wc2[cols])
            acc = part if acc is None else acc + part
            if do_a:
                pre = dot(v_cur[...], wc1[:, cols]) + 0.5 * bc1[layer:layer + 1, cols]
                act[:, cols] = gelu_of_half(pre).astype(BF16)
                for r in range(k * share, (k + 1) * share, STRIP):
                    prepare(v_next, after, slice(r, r + STRIP))
        z = (xb[before].astype(F32) + (acc + bc2[layer:layer + 1])).astype(BF16)
        return before, z

    load(first).wait()
    for r in range(0, rows, STRIP):
        prepare(v0, first * GROUP, slice(r, r + STRIP))
    for c in weights:
        c.wait()

    def scale(r, carry):
        at = pl.ds(pl.multiple_of(r * 64, 64), 64)
        wc1[at] = wc1[at] * jnp.asarray(0.5, BF16)
        return carry

    lax.fori_loop(0, chans // 64, scale, 0)
    for g in range(first):
        load(g).start()

    def pair(p, carry):
        g = first + p

        @pl.when(g + 1 < groups)
        def _():
            load(jnp.minimum(g + 1, groups - 1)).wait()

        before, z = unit(g * GROUP, v0, v1, True)

        @pl.when(p > 0)
        def _():
            xb[before] = z
            store(jnp.maximum(g - 1, first)).start()

        before, z = unit(g * GROUP + 1, v1, v0, True)
        xb[before] = z
        for n in range(pace):
            other = p * pace + n

            @pl.when(other < first)
            def _():
                load(jnp.minimum(other, first - 1)).wait()
                store(jnp.minimum(other, first - 1)).start()

        return carry

    lax.fori_loop(0, LEFT_OVER, pair, 0)
    before, z = unit(batch, v0, v1, False)
    xb[before] = z
    store(groups - 1).start()

    def drain(g, carry):
        store(g).wait()
        return carry

    lax.fori_loop(0, groups, drain, 0)


def solution(mesh):
    size = mesh.shape["seq"]
    chips = size // 2

    def local_layers(x, w_tok1, b_tok1, w_tok2, b_tok2, w_ch1, b_ch1, w_ch2, b_ch2, ln_params):
        layers = w_tok1.shape[0]
        batch, rows, chans = x.shape
        hid, wide = w_tok1.shape[2], w_ch1.shape[2]
        own = hid // size
        groups = batch // GROUP
        vmem = pl.BlockSpec(memory_space=pltpu.VMEM)
        hbm = pl.BlockSpec(memory_space=pl.ANY)
        tile = pltpu.VMEM((rows, chans), BF16)
        most = pl.pallas_call(
            functools.partial(kernel, chips),
            out_shape=jax.ShapeDtypeStruct(x.shape, BF16),
            in_specs=[hbm, hbm, vmem, hbm, vmem, hbm, vmem, hbm, vmem, vmem],
            out_specs=hbm,
            scratch_shapes=[
                pltpu.VMEM((batch + 1, rows, chans), BF16),
                pltpu.VMEM(w_ch1.shape, BF16),
                pltpu.VMEM(w_ch2.shape, BF16),
                pltpu.VMEM((rows, wide), BF16),
                tile, tile, tile, tile,
                pltpu.VMEM((HELD, GROUP, 2, chips, own, chans), F32),
                pltpu.VMEM((SLOTS, GROUP, chips, own, chans), F32),
                pltpu.VMEM((SLOTS, GROUP, chips, own, chans), F32),
                pltpu.VMEM((SLOTS, 2, GROUP, own // 2, chans), F32),
                pltpu.VMEM((SLOTS, 2, GROUP, own, chans), F32),
                pltpu.VMEM((SLOTS, GROUP, 2, chips, own, chans), BF16),
                pltpu.VMEM((layers, rows, hid), BF16),
                pltpu.VMEM((layers, hid, rows), BF16),
                pltpu.VMEM((layers, hid, rows), BF16),
                pltpu.VMEM((layers, rows, hid), BF16),
                pltpu.VMEM((layers, own, 1), F32),
                pltpu.VMEM((layers, rows, 1), F32),
                pltpu.SemaphoreType.DMA((groups,)),
                pltpu.SemaphoreType.DMA((5,)),
                pltpu.SemaphoreType.DMA((groups,)),
                pltpu.SemaphoreType.DMA((KINDS, SLOTS)),
                pltpu.SemaphoreType.DMA((KINDS, SLOTS)),
            ],
            compiler_params=pltpu.CompilerParams(
                collective_id=0, has_side_effects=True, vmem_limit_bytes=67043328),
        )(x, w_tok1, b_tok1, w_tok2, b_tok2, w_ch1, b_ch1, w_ch2, b_ch2, ln_params)
        return pl.pallas_call(
            last_kernel,
            out_shape=jax.ShapeDtypeStruct(x.shape, BF16),
            in_specs=[hbm, hbm, vmem, hbm, vmem, vmem],
            out_specs=hbm,
            scratch_shapes=[
                pltpu.VMEM(x.shape, BF16),
                pltpu.VMEM(w_ch1.shape[1:], BF16),
                pltpu.VMEM(w_ch2.shape[1:], BF16),
                pltpu.VMEM((rows, wide), BF16),
                tile, tile,
                pltpu.SemaphoreType.DMA((groups,)),
                pltpu.SemaphoreType.DMA((2,)),
                pltpu.SemaphoreType.DMA((groups,)),
            ],
            compiler_params=pltpu.CompilerParams(vmem_limit_bytes=67043328),
        )(most, w_ch1, b_ch1, w_ch2, b_ch2, ln_params)

    act = P("data", "seq", None)
    rep = P()
    return jax.shard_map(local_layers, mesh=mesh, in_specs=(act,) + (rep,) * 9, out_specs=act, check_vma=False)
```
